32 devices in a mesh: batch: 8 (over y, x, core), shard: 4 (over z).
Axes of the slice: x: 2, y: 2, z: 4, core: 2. Of those that a mesh axis runs over, the one named last changes fastest.
Arguments:
- particles: float32 [8192, 1024], P(('batch', 'shard')), may hold values from -48 to 48
- batch_of: int32 [2, 8192], P(None, ('batch', 'shard')), may hold values from 0 to 7, as said below
- mixture_means: float32 [16, 1024], replicated, may hold values from -3 to 3
- log_weights: float32 [16], replicated, may hold values from -2 to 2
Outputs:
- moved: float32 [8192, 1024], P(('batch', 'shard'))
The draws below stay inside these ranges and needn't reach their ends.
Inputs may be any that keep to these rules, and one draw needn't show every extreme that they name: `batch_of`: in each iteration, the 256 particles of one device hold every batch number equally often, 256 / 8 times each.
All inputs are finite; a program needn't handle non-finite values.
Results may differ from the reference program's by a relative error of at most 0.00011.
Values sent between devices are 32-bit elements; how exact they have to be, the bound alone decides.
A program may use at most 64 MiB of HBM per device.

```python
import jax
import jax.numpy as jnp
from jax import lax

D = 1024
COMPONENTS = 16
ITERS = 2
P_DEV = 256
BATCHES = 8
BATCH_ROWS = 1024
PARTICLES = 8192


def draw_particles(key, part):
    first, second = jax.random.split(key, 2)
    ranks = jax.random.permutation(second, D).astype(jnp.float32) + 1.0
    harmonic = jnp.sum(1.0 / (jnp.arange(D, dtype=jnp.float32) + 1.0))
    column_scale = jnp.sqrt(D / (harmonic * ranks))
    points = jax.random.normal(first, (PARTICLES, D), jnp.float32) * column_scale[None, :]
    return jnp.clip(points, -48.0, 48.0)


def draw_batch_of(key, part):
    devices = PARTICLES // P_DEV
    ranks = jax.random.randint(key, (ITERS, devices, P_DEV), 0, 2 ** 20) * P_DEV + jnp.arange(P_DEV, dtype=jnp.int32)
    ordering = jnp.argsort(ranks, axis=2, stable=True)
    return (ordering % BATCHES).reshape(ITERS, PARTICLES).astype(jnp.int32)


def gaussian(key, extent, width, most, kind=jnp.bfloat16):
    return jnp.clip(width * jax.random.normal(key, extent, jnp.float32), -most, most).astype(kind)


def setup_inputs(seed: int = 0) -> dict:
    streams_of = jax.random.split(jax.random.key(seed), 5)
    return {
        "particles": draw_particles(jax.random.fold_in(streams_of[4], 71), 0),
        "batch_of": draw_batch_of(jax.random.fold_in(streams_of[4], 71), 0),
        "mixture_means": gaussian(streams_of[2], (COMPONENTS, D), 0.5, 3.0, jnp.float32),
        "log_weights": jnp.clip(jax.random.uniform(streams_of[3], (COMPONENTS,), jnp.float32, -2.0, 2.0), -2.0, 2.0),
    }


variance = 4.0
step_size = 32.0


def mixture_score(points, mixture_means, log_weights):
    squares = jnp.sum(points * points, axis=1, keepdims=True)
    crossed = jnp.dot(points, mixture_means.T, precision=lax.Precision.HIGHEST, preferred_element_type=jnp.float32)
    centre_sq = jnp.sum(mixture_means * mixture_means, axis=1)
    logits = log_weights[None, :] - (squares - 2.0 * crossed + centre_sq[None, :]) / (2.0 * variance)
    weights_mix = jax.nn.softmax(logits, axis=1)
    pulled = jnp.dot(weights_mix, mixture_means, precision=lax.Precision.HIGHEST, preferred_element_type=jnp.float32)
    return (pulled - points) / variance


def group_drift(group, mixture_means, log_weights):
    scores = mixture_score(group, mixture_means, log_weights)
    squares = jnp.sum(group * group, axis=1)
    crossed = jnp.dot(group, group.T, precision=lax.Precision.HIGHEST, preferred_element_type=jnp.float32)
    kernel = jnp.exp(-(squares[:, None] + squares[None, :] - 2.0 * crossed) * (2.0 / D))
    acc_score = jnp.dot(kernel, scores, precision=lax.Precision.HIGHEST, preferred_element_type=jnp.float32)
    acc_point = jnp.dot(kernel, group, precision=lax.Precision.HIGHEST, preferred_element_type=jnp.float32)
    kernel_sum = jnp.sum(kernel, axis=1)
    return (acc_score + (4.0 / D) * (group * kernel_sum[:, None] - acc_point)) / BATCH_ROWS


def reference(particles, batch_of, mixture_means, log_weights):
    current = particles
    for iteration in range(ITERS):
        ordering = jnp.argsort(batch_of[iteration], stable=True).astype(jnp.int32)
        grouped = current[ordering].reshape(BATCHES, BATCH_ROWS, D)
        moved = lax.map(lambda group: group + step_size * group_drift(group, mixture_means, log_weights), grouped)
        current = jnp.zeros_like(current).at[ordering].set(moved.reshape(PARTICLES, D))
    return current
```

```python
import functools

import jax
import jax.numpy as jnp
from jax import lax
from jax.experimental import pallas as pl
from jax.experimental.pallas import tpu as pltpu
from jax.sharding import PartitionSpec as P

variance = 4.0
step_size = 32.0
PARTS = 2
MESH = pl.DeviceIdType.MESH
f32, bf16 = jnp.float32, jnp.bfloat16


def split(a):
    high = a.astype(bf16)
    return high, (a - high.astype(f32)).astype(bf16)


def dot(a, b, contract=((1,), (0,))):
    return lax.dot_general(a, b, (contract, ((), ())), preferred_element_type=f32)


def dot3(a, b, contract=((1,), (0,))):
    return dot(a[0], b[0], contract) + (dot(a[0], b[1], contract) + dot(a[1], b[0], contract))


def permute(matrix, rows):
    high, rest = rows.astype(bf16), None
    rest = rows - high.astype(f32)
    middle, low = split(rest)
    return dot(matrix, high) + (dot(matrix, middle) + dot(matrix, low))


def orders(batch, chunk):
    count = batch.shape[1]
    down = lax.broadcasted_iota(jnp.int32, (count, count), 0)
    along = lax.broadcasted_iota(jnp.int32, (count, count), 1)
    column = jnp.sum(jnp.where(down == along, batch, 0), axis=1, keepdims=True)
    same = column == batch
    rank_row = jnp.sum(jnp.where(same & (down < along), 1, 0), axis=0, keepdims=True)
    rank_column = jnp.sum(jnp.where(same & (along < down), 1, 0), axis=1, keepdims=True)
    there = jnp.where(down == batch * chunk + rank_row, 1.0, 0.0).astype(bf16)
    back = jnp.where(along == column * chunk + rank_column, 1.0, 0.0).astype(bf16)
    return there, back


def kernel(
    groups,
    shards,
    iters,
    x_ref,
    batch_ref,
    means_ref,
    logw_ref,
    out_ref,
    start,
    sent,
    pool,
    moved,
    home,
    final,
    x_high,
    x_low,
    k_high,
    k_low,
    lhs_high,
    lhs_low,
    own_sq,
    acc_w,
    acc_k,
    local_sem,
    a_send,
    a_recv,
    x_send,
    x_recv,
    c_send,
    c_recv,
    r_send,
    r_recv,
):
    count, width = x_ref.shape
    chunk = count // groups
    members = shards
    pairs = members // 2
    wide = groups // shards
    near = shards // 2
    parts = PARTS
    cols = width // parts
    b = lax.axis_index("batch")
    s = lax.axis_index("shard")
    q, t = b // members, b % members
    x, c = t // 2, t % 2
    g = q * shards + s
    side, l = s // near, s % near
    e = (1 - side) * (near - 1 - l) + side * l

    def shard_at(side_at, e_at):
        return (1 - side_at) * (near - 1 - e_at) + side_at * (near + e_at)

    def place(q_at, s_at):
        return q_at * members + t, s_at

    def mate(j, other):
        return q * members + lax.rem(x + j, pairs) * 2 + (1 - c if other else c), s

    def rows_of(index, size=chunk):
        return pl.ds(pl.multiple_of(index * size, 8), size)

    def part(p):
        return slice(p * cols, (p + 1) * cols)

    def slot(far, a, dq):
        return (far * near + a) * wide + dq

    slots = [(far, a, dq) for far in range(2) for a in range(near) for dq in range(wide)]

    def source(k):
        far, a, dq = slots[k]
        q_at = lax.rem(q + wide - dq, wide)
        if far:
            return q_at, shard_at(1 - side, a)
        return q_at, shard_at(side, lax.rem(e + a, near))

    def remote(src, dst, send, recv, device):
        return pltpu.make_async_remote_copy(
            src_ref=src, dst_ref=dst, send_sem=send, recv_sem=recv, device_id=device, device_id_type=MESH
        )

    load = pltpu.make_async_copy(x_ref, start, local_sem.at[0])
    load.start()
    barrier = pltpu.get_barrier_semaphore()
    targets = [place(*source(k)) for k in range(1, groups)]
    targets += [mate(j, False) for j in range(1, pairs)] + [mate(0, True)]
    for target in targets:
        pl.semaphore_signal(barrier, inc=1, device_id=target, device_id_type=MESH)

    logw = logw_ref[...]
    means = means_ref[...]
    mean_parts = split(means)
    mean_sq = jnp.sum(means * means, axis=1, keepdims=True)
    lhs_high[count:, :] = mean_parts[0]
    lhs_low[count:, :] = mean_parts[1]

    there, back = orders(batch_ref[0:1, :], chunk)
    load.wait()
    for p in range(parts):
        sent[0, :, part(p)] = permute(there, start[:, part(p)])
    pl.semaphore_wait(barrier, len(targets))

    def arrival(it, k, p):
        spot = pool.at[it, t, rows_of(k), part(p)]
        return remote(spot, spot, a_send.at[k, p], a_recv.at[k, p], place(*source(k)))

    def send_in(it, k_send, k_recv, q_at, s_at, p):
        to = q_at * shards + s_at
        copy = remote(
            sent.at[it, rows_of(to), part(p)],
            pool.at[it, t, rows_of(k_recv), part(p)],
            a_send.at[k_send, p],
            a_recv.at[k_recv, p],
            place(q_at, s_at),
        )
        copy.start()
        return copy

    def send_near(it, p):
        copies = []
        for r in range(near):
            for dq in range(wide):
                k = slot(0, r, dq)
                if k == 0:
                    pool[it, t, 0:chunk, part(p)] = sent[it, rows_of(g), part(p)]
                else:
                    s_at = shard_at(side, lax.rem(e + near - r, near))
                    copies.append(send_in(it, k, k, lax.rem(q + dq, wide), s_at, p))
        return copies

    def send_far(it, e_at, p):
        copies = []
        for dq in range(wide):
            k_recv = (near + e) * wide + dq
            copies.append(
                send_in(it, slot(1, e_at, dq), k_recv, lax.rem(q + dq, wide), shard_at(1 - side, e_at), p)
            )
        return copies

    def pass_on(it, j, k, p, other):
        block = lax.rem(x + pairs - (j if other else 0), pairs) * 2 + c
        spot = pool.at[it, block, rows_of(k), part(p)]
        sem = (c_send, c_recv) if other else (x_send, x_recv)
        copy = remote(
            spot, spot, sem[0].at[it, j, k, p], sem[1].at[it, j, k, p], mate(0, True) if other else mate(j, False)
        )
        copy.start()
        return copy

    def gather(it):
        half = groups // 2
        pieces = [(k, p) for p in range(parts) for k in range(half)]
        pieces += [(k, p) for p in range(parts) for k in range(half, groups)]
        lag = 2
        across, inside = {}, {}
        for n in range(len(pieces) + lag):
            if n < len(pieces):
                k, p = pieces[n]
                if k:
                    arrival(it, k, p).wait_recv()
                for j in range(1, pairs):
                    across[j, n] = pass_on(it, j, k, p, False)
                inside[0, n] = pass_on(it, 0, k, p, True)
            if n >= lag:
                for j in range(1, pairs):
                    across[j, n - lag].wait_recv()
                    inside[j, n - lag] = pass_on(it, j, *pieces[n - lag], True)
        for copy in inside.values():
            copy.wait_recv()
        return list(across.values()) + list(inside.values())

    def grams(it):
        own = pool[it, t]
        high, low = split(own)
        lhs_high[0:count, :] = high
        lhs_low[0:count, :] = low
        own_sq[...] = jnp.sum(own * own, axis=1, keepdims=True)
        acc_w[...] = jnp.zeros_like(acc_w)
        acc_k[...] = jnp.zeros_like(acc_k)

        def block(m, carry):
            points = pool[it, m]
            both = split(points)
            x_high[m] = both[0]
            x_low[m] = both[1]
            sq = jnp.sum(points * points, axis=1, keepdims=True)
            sq_row = jnp.transpose(jnp.broadcast_to(sq, (count, 128)))[0:1, :]
            crossed = dot3((lhs_high[...], lhs_low[...]), both, ((1,), (1,)))
            values = jnp.exp(-(own_sq[...] + sq_row - 2.0 * crossed[:count]) * (2.0 / width))
            logits = logw - (sq_row - 2.0 * crossed[count:] + mean_sq) / (2.0 * variance)
            weights = jnp.exp(logits - jnp.max(logits, axis=0, keepdims=True))
            weights = weights / jnp.sum(weights, axis=0, keepdims=True)
            pair = split(values)
            k_high[m] = pair[0]
            k_low[m] = pair[1]
            acc_w[...] += dot3(pair, split(weights), ((1,), (1,)))
            acc_k[...] += jnp.sum(values, axis=1, keepdims=True)
            return carry

        lax.fori_loop(0, members, block, 0)

    def send_back(it, p):
        total = None
        for m in range(members):
            pair = (k_high[m], k_low[m])
            one = dot3(pair, (x_high[m, :, part(p)], x_low[m, :, part(p)]))
            total = one if total is None else total + one
        pulled = dot3(split(acc_w[...]), (mean_parts[0][:, part(p)], mean_parts[1][:, part(p)]))
        rows = pool[it, t, :, part(p)]
        drift = (pulled - total) / variance + (4.0 / width) * (rows * acc_k[...] - total)
        moved[it, :, part(p)] = rows + (step_size / (count * members)) * drift
        copies = []
        for k in list(range(groups // 2, groups)) + list(range(1, groups // 2)):
            far, a, dq = slots[k]
            k_recv = (near + e) * wide + dq if far else k
            copy = remote(
                moved.at[it, rows_of(k), part(p)],
                home.at[it, rows_of(g), part(p)],
                r_send.at[k, p],
                r_recv.at[k_recv, p],
                place(*source(k)),
            )
            copy.start()
            copies.append(copy)
        home[it, rows_of(g), part(p)] = moved[it, 0:chunk, part(p)]
        return copies

    def wait_home(it, p):
        for k in range(1, groups):
            far, a, dq = slots[k]
            if far:
                q_at, s_at = lax.rem(q + dq, wide), shard_at(1 - side, a)
            else:
                q_at, s_at = lax.rem(q + dq, wide), shard_at(side, lax.rem(e + near - a, near))
            spot = home.at[it, rows_of(q_at * shards + s_at), part(p)]
            remote(spot, spot, r_send.at[k, p], r_recv.at[k, p], place(q_at, s_at)).wait_recv()

    sends = []
    for p in range(parts):
        sends += send_near(0, p)
    for e_at in range(near):
        for p in range(parts):
            sends += send_far(0, e_at, p)
    for it in range(iters):
        sends += gather(it)
        grams(it)
        returns = []
        for p in range(parts):
            returns += send_back(it, p)
        for copy in sends:
            copy.wait_send()
        sends = []
        last = it == iters - 1
        if not last:
            next_there, next_back = orders(batch_ref[it + 1 : it + 2, :], chunk)
            turn = dot(next_there, back).astype(bf16)
            back = next_back
        stores = []
        for p in range(parts):
            wait_home(it, p)
            block = home[it, :, part(p)]
            if last:
                final[:, part(p)] = permute(back, block)
                store = pltpu.make_async_copy(
                    final.at[:, part(p)], out_ref.at[:, part(p)], local_sem.at[1 + p]
                )
                store.start()
                stores.append(store)
            else:
                sent[it + 1, :, part(p)] = permute(turn, block)
                sends += send_near(it + 1, p)
                sends += send_far(it + 1, 0, p)
        if not last:
            for e_at in range(1, near):
                for p in range(parts):
                    sends += send_far(it + 1, e_at, p)
        for copy in returns:
            copy.wait_send()
        for store in stores:
            store.wait()


def body(particles, batch_of, mixture_means, log_weights):
    groups = lax.axis_size("batch")
    shards = lax.axis_size("shard")
    iters = batch_of.shape[0]
    count, width = particles.shape
    components = mixture_means.shape[0]
    pairs = shards // 2
    dma = pltpu.SemaphoreType.DMA
    vmem = pl.BlockSpec(memory_space=pltpu.VMEM)
    return pl.pallas_call(
        functools.partial(kernel, groups, shards, iters),
        out_shape=jax.ShapeDtypeStruct((count, width), f32),
        in_specs=[pl.BlockSpec(memory_space=pl.ANY), vmem, vmem, vmem],
        out_specs=pl.BlockSpec(memory_space=pl.ANY),
        scratch_shapes=[
            pltpu.VMEM((count, width), f32),
            pltpu.VMEM((iters, count, width), f32),
            pltpu.VMEM((iters, shards, count, width), f32),
            pltpu.VMEM((iters, count, width), f32),
            pltpu.VMEM((iters, count, width), f32),
            pltpu.VMEM((count, width), f32),
            pltpu.VMEM((shards, count, width), bf16),
            pltpu.VMEM((shards, count, width), bf16),
            pltpu.VMEM((shards, count, count), bf16),
            pltpu.VMEM((shards, count, count), bf16),
            pltpu.VMEM((count + components, width), bf16),
            pltpu.VMEM((count + components, width), bf16),
            pltpu.VMEM((count, 1), f32),
            pltpu.VMEM((count, components), f32),
            pltpu.VMEM((count, 1), f32),
            dma((1 + PARTS,)),
            dma((groups, PARTS)),
            dma((groups, PARTS)),
            dma((iters, pairs, groups, PARTS)),
            dma((iters, pairs, groups, PARTS)),
            dma((iters, pairs, groups, PARTS)),
            dma((iters, pairs, groups, PARTS)),
            dma((groups, PARTS)),
            dma((groups, PARTS)),
        ],
        compiler_params=pltpu.CompilerParams(
            collective_id=0, has_side_effects=True, vmem_limit_bytes=58 * 1024 * 1024
        ),
    )(particles, batch_of, mixture_means, log_weights[:, None])


def solution(mesh):
    placed = (P(("batch", "shard"), None), P(None, ("batch", "shard")), P(), P())
    return jax.shard_map(
        body, mesh=mesh, in_specs=placed, out_specs=P(("batch", "shard"), None), check_vma=False
    )
```

```python
import functools

import jax
import jax.numpy as jnp
from jax import lax
from jax.experimental import pallas as pl
from jax.experimental.pallas import tpu as pltpu
from jax.sharding import PartitionSpec as P

variance = 4.0
step_size = 32.0
PARTS = 2
LAG = 6
MESH = pl.DeviceIdType.MESH
f32, bf16 = jnp.float32, jnp.bfloat16


def split(a):
    high = a.astype(bf16)
    return high, (a - high.astype(f32)).astype(bf16)


def dot(a, b, contract=((1,), (0,))):
    return lax.dot_general(a, b, (contract, ((), ())), preferred_element_type=f32)


def dot3(a, b, contract=((1,), (0,))):
    return dot(a[0], b[0], contract) + (dot(a[0], b[1], contract) + dot(a[1], b[0], contract))


def permute(matrix, rows):
    high, rest = rows.astype(bf16), None
    rest = rows - high.astype(f32)
    middle, low = split(rest)
    return dot(matrix, high) + (dot(matrix, middle) + dot(matrix, low))


def orders(batch, chunk):
    count = batch.shape[1]
    down = lax.broadcasted_iota(jnp.int32, (count, count), 0)
    along = lax.broadcasted_iota(jnp.int32, (count, count), 1)
    column = jnp.sum(jnp.where(down == along, batch, 0), axis=1, keepdims=True)
    same = column == batch
    rank_row = jnp.sum(jnp.where(same & (down < along), 1, 0), axis=0, keepdims=True)
    rank_column = jnp.sum(jnp.where(same & (along < down), 1, 0), axis=1, keepdims=True)
    there = jnp.where(down == batch * chunk + rank_row, 1.0, 0.0).astype(bf16)
    back = jnp.where(along == column * chunk + rank_column, 1.0, 0.0).astype(bf16)
    return there, back


def kernel(
    groups,
    shards,
    iters,
    x_ref,
    batch_hbm,
    means_hbm,
    logw_hbm,
    final,
    batch_ref,
    means_ref,
    logw_ref,
    start,
    sent,
    pool,
    moved,
    home,
    x_high,
    x_low,
    k_high,
    k_low,
    lhs_high,
    lhs_low,
    own_sq,
    acc_w,
    acc_k,
    local_sem,
    a_send,
    a_recv,
    x_send,
    x_recv,
    c_send,
    c_recv,
    r_send,
    r_recv,
):
    count, width = x_ref.shape
    chunk = count // groups
    members = shards
    pairs = members // 2
    wide = groups // shards
    near = shards // 2
    parts = PARTS
    cols = width // parts
    b = lax.axis_index("batch")
    s = lax.axis_index("shard")
    q, t = b // members, b % members
    x, c = t // 2, t % 2
    g = q * shards + s
    side, l = s // near, s % near
    e = (1 - side) * (near - 1 - l) + side * l

    def shard_at(side_at, e_at):
        return (1 - side_at) * (near - 1 - e_at) + side_at * (near + e_at)

    def place(q_at, s_at):
        return q_at * members + t, s_at

    def mate(j, other):
        return q * members + lax.rem(x + j, pairs) * 2 + (1 - c if other else c), s

    def rows_of(index, size=chunk):
        return pl.ds(pl.multiple_of(index * size, 8), size)

    def part(p):
        return slice(p * cols, (p + 1) * cols)

    def slot(far, a, dq):
        return (far * near + a) * wide + dq

    slots = [(far, a, dq) for far in range(2) for a in range(near) for dq in range(wide)]

    def source(k):
        far, a, dq = slots[k]
        if far:
            return lax.rem(q + wide - dq, wide), shard_at(1 - side, a)
        return lax.rem(q + wide - dq, wide), shard_at(side, lax.rem(e + a, near))

    def remote(src, dst, send, recv, device):
        return pltpu.make_async_remote_copy(
            src_ref=src, dst_ref=dst, send_sem=send, recv_sem=recv, device_id=device, device_id_type=MESH
        )

    pairs_of = ((x_ref, start), (batch_hbm, batch_ref), (means_hbm, means_ref), (logw_hbm, logw_ref))
    loads = [pltpu.make_async_copy(src, dst, local_sem.at[n]) for n, (src, dst) in enumerate(pairs_of)]
    for load in loads:
        load.start()
    barrier = pltpu.get_barrier_semaphore()
    targets = [place(*source(k)) for k in range(1, groups)]
    targets += [mate(j, False) for j in range(1, pairs)] + [mate(0, True)]
    for target in targets:
        pl.semaphore_signal(barrier, inc=1, device_id=target, device_id_type=MESH)

    loads[1].wait()
    there, back = orders(batch_ref[0:1, :], chunk)
    loads[0].wait()
    for p in range(parts):
        sent[0, :, part(p)] = permute(there, start[:, part(p)])
    loads[2].wait()
    loads[3].wait()
    means = means_ref[...]
    components = means.shape[0]
    down = lax.broadcasted_iota(jnp.int32, (components, components), 0)
    along = lax.broadcasted_iota(jnp.int32, (components, components), 1)
    logw = jnp.sum(jnp.where(down == along, logw_ref[...], 0.0), axis=1, keepdims=True)
    mean_parts = split(means)
    mean_sq = jnp.sum(means * means, axis=1, keepdims=True)
    lhs_high[count:, :] = mean_parts[0]
    lhs_low[count:, :] = mean_parts[1]

    pl.semaphore_wait(barrier, len(targets))

    def arrival(it, k, p):
        spot = pool.at[it, t, rows_of(k), part(p)]
        return remote(spot, spot, a_send.at[k, p], a_recv.at[k, p], place(*source(k)))

    def send_in(it, k_send, k_recv, q_at, s_at, p):
        to = q_at * shards + s_at
        copy = remote(
            sent.at[it, rows_of(to), part(p)],
            pool.at[it, t, rows_of(k_recv), part(p)],
            a_send.at[k_send, p],
            a_recv.at[k_recv, p],
            place(q_at, s_at),
        )
        copy.start()
        return copy

    def send_near(it, p):
        copies = []
        for r in range(near):
            for dq in range(wide):
                k = slot(0, r, dq)
                if k == 0:
                    pool[it, t, 0:chunk, part(p)] = sent[it, rows_of(g), part(p)]
                else:
                    s_at = shard_at(side, lax.rem(e + near - r, near))
                    copies.append(send_in(it, k, k, lax.rem(q + dq, wide), s_at, p))
        return copies

    def send_far(it, e_at, p):
        copies = []
        for dq in range(wide):
            k_recv = (near + e) * wide + dq
            copies.append(
                send_in(it, slot(1, e_at, dq), k_recv, lax.rem(q + dq, wide), shard_at(1 - side, e_at), p)
            )
        return copies

    def pass_on(it, j, k, p, other):
        block = lax.rem(x + pairs - (j if other else 0), pairs) * 2 + c
        spot = pool.at[it, block, rows_of(k), part(p)]
        sem = (c_send, c_recv) if other else (x_send, x_recv)
        copy = remote(
            spot, spot, sem[0].at[it, j, k, p], sem[1].at[it, j, k, p], mate(0, True) if other else mate(j, False)
        )
        copy.start()
        return copy

    def gather(it):
        half = groups // 2
        pieces = [(k, p) for p in range(parts) for k in range(half)]
        pieces += [(k, p) for p in range(parts) for k in range(half, groups)]
        if it == 0:
            pieces = [(0, p) for p in range(parts)] + [(k, p) for p in range(parts) for k in range(1, half)]
            pieces += [(slot(1, a, dq), p) for a in range(near) for p in range(parts) for dq in range(wide)]
        across, inside = {}, {}

        def pass_inside(n):
            for j in range(1, pairs):
                across[j, n].wait_recv()
                inside[j, n] = pass_on(it, j, *pieces[n], True)

        for n, (k, p) in enumerate(pieces):
            if k:
                arrival(it, k, p).wait_recv()
            for j in range(1, pairs):
                across[j, n] = pass_on(it, j, k, p, False)
            inside[0, n] = pass_on(it, 0, k, p, True)
            if n >= LAG:
                pass_inside(n - LAG)

        own = pool[it, t]
        high, low = split(own)
        lhs_high[0:count, :] = high
        lhs_low[0:count, :] = low
        own_sq[...] = jnp.sum(own * own, axis=1, keepdims=True)
        acc_w[...] = jnp.zeros_like(acc_w)
        acc_k[...] = jnp.zeros_like(acc_k)

        def block(m):
            points = pool[it, m]
            both = split(points)
            x_high[m] = both[0]
            x_low[m] = both[1]
            sq = jnp.sum(points * points, axis=1, keepdims=True)
            sq_row = jnp.transpose(jnp.broadcast_to(sq, (count, 128)))[0:1, :]
            crossed = dot3((lhs_high[...], lhs_low[...]), both, ((1,), (1,)))
            values = jnp.exp(-(own_sq[...] + sq_row - 2.0 * crossed[:count]) * (2.0 / width))
            logits = logw - (sq_row - 2.0 * crossed[count:] + mean_sq) / (2.0 * variance)
            weights = jnp.exp(logits - jnp.max(logits, axis=0, keepdims=True))
            weights = weights / jnp.sum(weights, axis=0, keepdims=True)
            pair = split(values)
            k_high[m] = pair[0]
            k_low[m] = pair[1]
            acc_w[...] += dot3(pair, split(weights), ((1,), (1,)))
            acc_k[...] += jnp.sum(values, axis=1, keepdims=True)

        def blocks(core):
            def one(j, carry):
                block(lax.rem(x + pairs - j, pairs) * 2 + core)
                return carry

            lax.fori_loop(1, pairs, one, 0)

        block(t)
        for n in range(len(pieces)):
            inside[0, n].wait_recv()
        block(x * 2 + 1 - c)
        for n in range(len(pieces) - LAG, len(pieces)):
            pass_inside(n)
        blocks(c)
        for (j, n), copy in inside.items():
            if j:
                copy.wait_recv()
        blocks(1 - c)
        return list(across.values()) + list(inside.values())

    def send_back(it, p):
        total = None
        for m in range(members):
            pair = (k_high[m], k_low[m])
            one = dot3(pair, (x_high[m, :, part(p)], x_low[m, :, part(p)]))
            total = one if total is None else total + one
        pulled = dot3(split(acc_w[...]), (mean_parts[0][:, part(p)], mean_parts[1][:, part(p)]))
        rows = pool[it, t, :, part(p)]
        drift = (pulled - total) / variance + (4.0 / width) * (rows * acc_k[...] - total)
        moved[it, :, part(p)] = rows + (step_size / (count * members)) * drift
        copies = []
        fars, nears = list(range(groups // 2, groups)), list(range(1, groups // 2))
        for k in fars + nears:
            far, a, dq = slots[k]
            k_recv = (near + e) * wide + dq if far else k
            copy = remote(
                moved.at[it, rows_of(k), part(p)],
                home.at[it, rows_of(g), part(p)],
                r_send.at[k, p],
                r_recv.at[k_recv, p],
                place(*source(k)),
            )
            copy.start()
            copies.append(copy)
        home[it, rows_of(g), part(p)] = moved[it, 0:chunk, part(p)]
        return copies

    def wait_home(it, p):
        for k in range(1, groups):
            far, a, dq = slots[k]
            if far:
                q_at, s_at = lax.rem(q + dq, wide), shard_at(1 - side, a)
            else:
                q_at, s_at = lax.rem(q + dq, wide), shard_at(side, lax.rem(e + near - a, near))
            spot = home.at[it, rows_of(q_at * shards + s_at), part(p)]
            remote(spot, spot, r_send.at[k, p], r_recv.at[k, p], place(q_at, s_at)).wait_recv()

    sends = []
    for p in range(parts):
        sends += send_near(0, p)
    for e_at in range(near):
        for p in range(parts):
            sends += send_far(0, e_at, p)
    for it in range(iters):
        sends += gather(it)
        returns = []
        for p in range(parts):
            returns += send_back(it, p)
        for copy in sends:
            copy.wait_send()
        sends = []
        last = it == iters - 1
        if not last:
            next_there, next_back = orders(batch_ref[it + 1 : it + 2, :], chunk)
            turn = dot(next_there, back).astype(bf16)
            back = next_back
        for p in range(parts):
            wait_home(it, p)
            block = home[it, :, part(p)]
            if last:
                final[:, part(p)] = permute(back, block)
            else:
                sent[it + 1, :, part(p)] = permute(turn, block)
                sends += send_near(it + 1, p)
                sends += send_far(it + 1, 0, p)
        if not last:
            for e_at in range(1, near):
                for p in range(parts):
                    sends += send_far(it + 1, e_at, p)
        for copy in returns:
            copy.wait_send()


def body(particles, batch_of, mixture_means, log_weights):
    groups = lax.axis_size("batch")
    shards = lax.axis_size("shard")
    iters = batch_of.shape[0]
    count, width = particles.shape
    components = mixture_means.shape[0]
    pairs = shards // 2
    dma = pltpu.SemaphoreType.DMA
    vmem = pl.BlockSpec(memory_space=pltpu.VMEM)
    return pl.pallas_call(
        functools.partial(kernel, groups, shards, iters),
        out_shape=jax.ShapeDtypeStruct((count, width), f32),
        in_specs=[pl.BlockSpec(memory_space=pl.ANY)] * 4,
        out_specs=pl.BlockSpec(memory_space=pltpu.VMEM),
        scratch_shapes=[
            pltpu.VMEM(batch_of.shape, jnp.int32),
            pltpu.VMEM(mixture_means.shape, f32),
            pltpu.VMEM((1, components), f32),
            pltpu.VMEM((count, width), f32),
            pltpu.VMEM((iters, count, width), f32),
            pltpu.VMEM((iters, shards, count, width), f32),
            pltpu.VMEM((iters, count, width), f32),
            pltpu.VMEM((iters, count, width), f32),
            pltpu.VMEM((shards, count, width), bf16),
            pltpu.VMEM((shards, count, width), bf16),
            pltpu.VMEM((shards, count, count), bf16),
            pltpu.VMEM((shards, count, count), bf16),
            pltpu.VMEM((count + components, width), bf16),
            pltpu.VMEM((count + components, width), bf16),
            pltpu.VMEM((count, 1), f32),
            pltpu.VMEM((count, components), f32),
            pltpu.VMEM((count, 1), f32),
            dma((4,)),
            dma((groups, PARTS)),
            dma((groups, PARTS)),
            dma((iters, pairs, groups, PARTS)),
            dma((iters, pairs, groups, PARTS)),
            dma((iters, pairs, groups, PARTS)),
            dma((iters, pairs, groups, PARTS)),
            dma((groups, PARTS)),
            dma((groups, PARTS)),
        ],
        compiler_params=pltpu.CompilerParams(
            collective_id=0, has_side_effects=True, vmem_limit_bytes=58 * 1024 * 1024
        ),
    )(particles, batch_of, mixture_means, log_weights[None, :])


def solution(mesh):
    placed = (P(("batch", "shard"), None), P(None, ("batch", "shard")), P(), P())
    return jax.shard_map(
        body, mesh=mesh, in_specs=placed, out_specs=P(("batch", "shard"), None), check_vma=False
    )
```
